32 devices in a mesh: task: 16 (over z, x, core), tensor: 2 (over y).
Axes of the slice: x: 2, y: 2, z: 4, core: 2. Of those that a mesh axis runs over, the one named last changes fastest.
Arguments:
- inputs: bfloat16 [2048, 4096], P('task', 'tensor'), may hold values from -6 to 6
- targets: bfloat16 [2048, 4096], P('task', 'tensor'), may hold values from -6 to 6
- queries: bfloat16 [2048, 2048], P('task', 'tensor'), may hold values from -120 to 120
- key_rows: bfloat16 [2048, 2048], P('task', 'tensor'), may hold values from -4 to 4
- value_weight: bfloat16 [4096, 2048], P(None, 'tensor'), may hold values from -0.09375 to 0.09375
- output_weight: bfloat16 [2048, 4096], P('tensor'), may hold values from -0.125 to 0.125
- splits: int32 [16], P('task'), may hold values from 32 to 96
Outputs:
- meta_value: float32 [4096, 2048], P('task', 'tensor')
- meta_output: float32 [2048, 4096], P('tensor', 'task')
The draws below stay inside these ranges and needn't reach their ends.
Inputs may be any that keep to these rules, and one draw needn't show every extreme that they name: `splits`: support and query parts of every task are both nonempty.
All inputs are finite; a program needn't handle non-finite values.
Results may differ from the reference program's by a relative error of at most 0.025.
Values may be sent and summed in bfloat16 or wider, within the bound.
A program may use at most 128 MiB of HBM per device.

```python
import jax
import jax.numpy as jnp
from jax import lax

D = 4096
HD = 128
HEADS = 16
INNER = 1
TASKS_DEV = 1
TASK_LEN = 128
TOKENS = 2048
N_TASK = 16
N_TENSOR = 2


def paired(key):
    first, second = jax.random.split(jax.random.fold_in(key, 7), 2)
    query_base = jnp.clip(jax.random.normal(first, (TOKENS, HEADS * HD), jnp.float32), -4.0, 4.0)
    key_base = jnp.clip(jax.random.normal(second, (TOKENS, HEADS * HD), jnp.float32), -4.0, 4.0)
    return (query_base, key_base)


def draw_queries(key, part):
    return paired(key)[0].astype(jnp.bfloat16)


def draw_key_rows(key, part):
    return paired(key)[1].astype(jnp.bfloat16)


def touch_ends(values, own_key, smallest, high):
    extent = values.shape
    place = [jax.random.randint(jax.random.fold_in(own_key, axis), (), 0, extent[axis]) for axis in range(len(extent))]
    values = values.at[tuple(place)].set(smallest)
    longest = extent.index(max(extent))
    place[longest] = (place[longest] + 1) % extent[longest]
    return values.at[tuple(place)].set(high)


def spiked(drawn, stream_key, source, target, blocks, factor):
    def block_of(dim):
        return (jnp.arange(drawn.shape[dim]) // (drawn.shape[dim] // blocks)).reshape((-1,) + (1,) * (drawn.ndim - 1 - dim))

    one_side = jax.random.permutation(stream_key, blocks)[block_of(target)]
    second = (block_of(target) + blocks // 2) % blocks
    return jnp.where((block_of(source) == one_side) | (block_of(source) == second), factor * drawn, drawn)


def steps_of(own_key, shape, cuts, low, top_value):
    level, own = 1.0, jax.random.fold_in(own_key, 6)
    for dim, blocks in cuts:
        heights = jnp.exp(jax.random.uniform(jax.random.fold_in(own, dim), (blocks,), jnp.float32, low / len(cuts), top_value / len(cuts)))
        level = level * jnp.repeat(heights, shape[dim] // blocks).reshape([-1 if axis == dim else 1 for axis in range(len(shape))])
    return level


def bell_draw(own_key, extent, scale, reach, pieces=(), kind=jnp.bfloat16):
    array = jax.random.normal(own_key, extent, jnp.float32) * scale
    if len(pieces) > 0:
        array = steps_of(own_key, extent, pieces, -0.22, 0.18) * array
    return jnp.clip(array, min=-reach, max=reach).astype(kind)


def gaussian_with(stream_key, shape, scale, most, shards, heavy, held_as=jnp.bfloat16):
    entries = scale * jax.random.normal(stream_key, shape, jnp.float32)
    if shards:
        entries = entries * steps_of(stream_key, shape, shards, -0.22, 0.18)
    return jnp.clip(spiked(entries, jax.random.fold_in(stream_key, 3), *heavy), -most, most).astype(held_as)


def setup_inputs(seed: int = 0) -> dict:
    streams_of = jax.random.split(jax.random.key(seed), 8)
    return {
        "inputs": gaussian_with(streams_of[0], (TOKENS, D), 1.0, 6.0, ((0, 16), (1, 2)), (0, 1, 16, 2.0)),
        "targets": bell_draw(streams_of[1], (TOKENS, D), 1.0, 6.0, ((0, 16), (1, 2))),
        "queries": draw_queries(jax.random.fold_in(streams_of[7], 71), 0),
        "key_rows": draw_key_rows(jax.random.fold_in(streams_of[7], 71), 0),
        "value_weight": bell_draw(streams_of[4], (D, HEADS * HD), D ** -0.5, 0.09375, ((1, 2),)),
        "output_weight": bell_draw(streams_of[5], (HEADS * HD, D), (HEADS * HD) ** -0.5, 0.125, ((0, 2),)),
        "splits": touch_ends(jax.random.randint(streams_of[6], (TASKS_DEV * N_TASK,), TASK_LEN // 4, 3 * TASK_LEN // 4 + 1), jax.random.fold_in(streams_of[6], 1), TASK_LEN // 4, (3 * TASK_LEN // 4 + 1) - 1).astype(jnp.int32),
    }


step_rate = 0.25

def normed_rows(inputs):
    values = inputs.astype(jnp.float32)
    scale = lax.rsqrt(lax.optimization_barrier(jnp.mean(values * values, axis=-1, keepdims=True)) + 1e-05)
    return (values * scale).astype(jnp.bfloat16)

def attention_probs(queries, key_rows, heads):
    length = queries.shape[0]
    query_f = queries.astype(jnp.float32).reshape(length, heads, -1)
    key_f = key_rows.astype(jnp.float32).reshape(length, heads, -1)
    scores = jnp.einsum('ihd,jhd->hij', query_f, key_f) / jnp.sqrt(jnp.float32(query_f.shape[2]))
    position = jnp.arange(length)
    causal = position[:, None] >= position[None, :]
    scores = jnp.where(causal[None], scores, jnp.float32(-1e+30))
    scores = scores - lax.optimization_barrier(jnp.max(scores, axis=-1, keepdims=True))
    expo = jnp.exp(scores)
    return (expo / lax.optimization_barrier(jnp.sum(expo, axis=-1, keepdims=True))).astype(jnp.bfloat16)

def local_out(value_mat, output_mat, normed, probs):
    heads = probs.shape[0]
    length = normed.shape[0]
    upper = jnp.dot(normed, value_mat.astype(jnp.bfloat16), preferred_element_type=jnp.float32).astype(jnp.bfloat16)
    mixed = jnp.einsum('hij,jhd->ihd', probs.astype(jnp.float32), upper.astype(jnp.float32).reshape(length, heads, -1))
    mixed = mixed.reshape(length, -1).astype(jnp.bfloat16)
    return jnp.dot(mixed, output_mat.astype(jnp.bfloat16), preferred_element_type=jnp.float32).astype(jnp.bfloat16)

def task_meta(value_mat, output_mat, inputs, targets, queries, key_rows, split):
    cols = HEADS * HD // N_TENSOR
    group = HEADS // N_TENSOR
    normed = normed_rows(inputs)
    probs = attention_probs(queries, key_rows, HEADS)
    position = jnp.arange(TASK_LEN)
    support = (position < split).astype(jnp.float32)[:, None]
    query_mask = 1.0 - support
    count_s = split.astype(jnp.float32)
    count_q = jnp.float32(TASK_LEN) - count_s
    input_f = inputs.astype(jnp.float32)
    target_f = targets.astype(jnp.float32)

    def total(value_now, output_now):
        result = input_f
        for index in range(N_TENSOR):
            result = result + local_out(value_now[:, index * cols:(index + 1) * cols], output_now[index * cols:(index + 1) * cols], normed, probs[index * group:(index + 1) * group]).astype(jnp.float32)
        return result

    def loss(value_now, output_now, mask, count):
        error = total(value_now, output_now) - target_f
        return 0.5 * jnp.sum(mask * error * error) / count

    def meta_loss(value_now, output_now):
        for inner in range(INNER):
            grad_value, grad_output = jax.grad(loss, argnums=(0, 1))(value_now, output_now, support, count_s)
            value_now = value_now - step_rate * grad_value
            output_now = output_now - step_rate * grad_output
        return loss(value_now, output_now, query_mask, count_q)
    return jax.grad(meta_loss, argnums=(0, 1))(value_mat, output_mat)

def reference(inputs, targets, queries, key_rows, value_weight, output_weight, splits):
    count = N_TASK * TASKS_DEV
    value_f = value_weight.astype(jnp.float32)
    output_f = output_weight.astype(jnp.float32)
    items = (inputs.reshape(count, TASK_LEN, D), targets.reshape(count, TASK_LEN, D), queries.reshape(count, TASK_LEN, HEADS * HD), key_rows.reshape(count, TASK_LEN, HEADS * HD), splits.astype(jnp.int32))

    def accumulate(carry, item):
        grad_value, grad_output = task_meta(value_f, output_f, item[0], item[1], item[2], item[3], item[4])
        return ((carry[0] + grad_value, carry[1] + grad_output), None)
    start = (jnp.zeros((D, HEADS * HD), jnp.float32), jnp.zeros((HEADS * HD, D), jnp.float32))
    result, unused = lax.scan(accumulate, start, items)
    return (result[0], result[1])
```

```python
import functools

import jax
import jax.numpy as jnp
from jax import lax
from jax.experimental import pallas as pl
from jax.experimental.pallas import tpu as pltpu
from jax.sharding import PartitionSpec as P

HD = 128
BF = jnp.bfloat16
F32 = jnp.float32

step_rate = 0.25


def normed_rows(inputs):
    values = inputs.astype(F32)
    scale = lax.rsqrt(jnp.mean(values * values, axis=-1, keepdims=True) + 1e-05)
    return (values * scale).astype(BF)


def attention_probs(queries, key_rows, heads):
    length = queries.shape[0]
    query_h = queries.reshape(length, heads, -1)
    key_h = key_rows.reshape(length, heads, -1)
    scores = jnp.einsum("ihd,jhd->hij", query_h, key_h, preferred_element_type=F32)
    scores = scores / jnp.sqrt(F32(query_h.shape[2]))
    position = jnp.arange(length)
    causal = position[:, None] >= position[None, :]
    scores = jnp.where(causal[None], scores, F32(-1e30))
    scores = scores - jnp.max(scores, axis=-1, keepdims=True)
    expo = jnp.exp(scores)
    return (expo / jnp.sum(expo, axis=-1, keepdims=True)).astype(BF)


def mm(left, right):
    return jnp.dot(left, right, preferred_element_type=F32)


def mm_nt(left, right):
    return lax.dot_general(left, right, (((1,), (1,)), ((), ())), preferred_element_type=F32)


def mm_tn(left, right):
    return lax.dot_general(left, right, (((0,), (0,)), ((), ())), preferred_element_type=F32)


def mix(probs, rows):
    heads = probs.shape[0]
    split = rows.reshape(rows.shape[0], heads, -1)
    out = jnp.einsum("hij,jhd->ihd", probs, split, preferred_element_type=F32)
    return out.reshape(out.shape[0], -1)


def mix_back(probs, rows):
    heads = probs.shape[0]
    split = rows.reshape(rows.shape[0], heads, -1)
    out = jnp.einsum("hij,ihd->jhd", probs, split, preferred_element_type=F32)
    return out.reshape(out.shape[0], -1)


def group_sum(term, count):
    term = term.astype(BF)
    if count == 1:
        return term.astype(F32)
    if count == 2:
        other = lax.ppermute(term, "tensor", ((0, 1), (1, 0)))
        return term.astype(F32) + other.astype(F32)
    share = lax.psum_scatter(term, "tensor", scatter_dimension=1, tiled=True)
    return lax.all_gather(share, "tensor", axis=1, tiled=True).astype(F32)


def full_rows(inputs, count, index):
    if count != 2:
        return lax.all_gather(inputs, "tensor", axis=1, tiled=True)
    other = lax.ppermute(inputs, "tensor", ((0, 1), (1, 0)))
    low = jnp.where(index == 0, inputs, other)
    high = jnp.where(index == 0, other, inputs)
    return jnp.concatenate([low, high], axis=1)


def gather_kernel(lines, src_ref, out_ref, own_sem, send_sem, line_sem, side_sem, core_sem):
    me = lax.axis_index("task")
    core, side, line = lax.rem(me, 2), lax.rem(me // 2, 2), me // 4

    def place(back, over_side, over_core):
        line_from = lax.rem(line + lines - back, lines)
        side_from = 1 - side if over_side else side
        core_from = 1 - core if over_core else core
        return (line_from * 2 + side_from) * 2 + core_from

    side_peer, core_peer = place(0, True, False), place(0, False, True)
    peers = [place(lines - step, False, False) for step in range(1, lines)] + [side_peer, core_peer]
    barrier = pltpu.get_barrier_semaphore()
    for peer in peers:
        pl.semaphore_signal(
            barrier, inc=1, device_id={"task": peer}, device_id_type=pl.DeviceIdType.MESH
        )
    pl.semaphore_wait(barrier, len(peers))

    started = []

    def send(source, slot, arrival, peer):
        copy = pltpu.make_async_remote_copy(
            src_ref=source,
            dst_ref=out_ref.at[slot],
            send_sem=send_sem.at[len(started)],
            recv_sem=arrival,
            device_id={"task": peer},
            device_id_type=pl.DeviceIdType.MESH,
        )
        copy.start()
        started.append(copy)

    def arrived(slot, arrival, peer):
        pltpu.make_async_remote_copy(
            src_ref=out_ref.at[slot],
            dst_ref=out_ref.at[slot],
            send_sem=send_sem.at[0],
            recv_sem=arrival,
            device_id={"task": peer},
            device_id_type=pl.DeviceIdType.MESH,
        ).wait_recv()

    for step in sorted(range(1, lines), key=lambda step: -min(step, lines - step)):
        send(src_ref, me, line_sem.at[step], peers[step - 1])
    send(src_ref, me, side_sem.at[0], side_peer)
    send(src_ref, me, core_sem.at[0, 0], core_peer)
    own = pltpu.make_async_copy(src_ref, out_ref.at[me], own_sem)
    own.start()
    order = sorted(range(1, lines), key=lambda step: min(step, lines - step))
    for step in order:
        slot = place(step, False, False)
        arrived(slot, line_sem.at[step], side_peer)
        send(out_ref.at[slot], slot, side_sem.at[step], side_peer)
        send(out_ref.at[slot], slot, core_sem.at[step, 0], core_peer)
    for step in [0] + order:
        slot = place(step, True, False)
        arrived(slot, side_sem.at[step], side_peer)
        send(out_ref.at[slot], slot, core_sem.at[step, 1], core_peer)
    for step in [0] + order:
        for over in range(2):
            arrived(place(step, over == 1, True), core_sem.at[step, over], core_peer)
    own.wait()
    for copy in started:
        copy.wait_send()


def gather_by_copies(rows, number):
    count = lax.axis_size("task")
    if count % 4:
        return gather_tokens(rows)
    lines = count // 4
    sends = (lines + 1) + 2 * (lines - 1) + lines
    gathered = pl.pallas_call(
        functools.partial(gather_kernel, lines),
        out_shape=jax.ShapeDtypeStruct((count,) + rows.shape, rows.dtype),
        in_specs=[pl.BlockSpec(memory_space=pltpu.VMEM)],
        out_specs=pl.BlockSpec(memory_space=pltpu.VMEM),
        scratch_shapes=[
            pltpu.SemaphoreType.DMA,
            pltpu.SemaphoreType.DMA((sends,)),
            pltpu.SemaphoreType.DMA((lines,)),
            pltpu.SemaphoreType.DMA((lines,)),
            pltpu.SemaphoreType.DMA((lines, 2)),
        ],
        compiler_params=pltpu.CompilerParams(collective_id=number, has_side_effects=True),
        cost_estimate=pl.CostEstimate(
            flops=0, bytes_accessed=16 * rows.size * rows.dtype.itemsize * count, transcendentals=0
        ),
    )(rows)
    return gathered.reshape(count * rows.shape[0], rows.shape[1])


def gather_tokens(rows):
    return lax.all_gather(rows, "task", axis=0, tiled=True)


def my_columns(rows):
    return lax.all_to_all(rows, "task", split_axis=1, concat_axis=0, tiled=True)


def below(rows, length):
    return jnp.pad(rows, ((0, length - rows.shape[0]), (0, 0)))


def above(rows, length):
    return jnp.pad(rows, ((length - rows.shape[0], 0), (0, 0)))


def make_device(tensor_count):
    def per_device(inputs, targets, queries, key_rows, value_weight, output_weight, splits):
        length = inputs.shape[0]
        low, high = length // 4, 3 * length // 4
        heads = queries.shape[1] // HD
        index = lax.axis_index("tensor")
        normed = normed_rows(full_rows(inputs, tensor_count, index))
        offset_here = inputs.astype(F32) - targets.astype(F32)
        offset = jnp.concatenate(
            [jnp.where(index == block, offset_here, F32(0.0)) for block in range(tensor_count)],
            axis=1,
        )
        probs = attention_probs(queries, key_rows, heads)
        probs_s = probs[:, :high, :high]
        probs_q = probs[:, low:, :]
        split = splits[0]
        count_s = split.astype(F32)
        position = jnp.arange(length)
        support = (position < split).astype(F32)[:, None]
        weight_s = (support / count_s)[:high]
        weight_q = ((1.0 - support) / (F32(length) - count_s))[low:]

        upper = mm(normed, value_weight).astype(BF)
        mixed_s = mix(probs_s, upper[:high]).astype(BF)
        gram = mm_nt(normed, normed).astype(BF)
        mixed_s_all = gather_tokens(mixed_s)
        part_0 = (mm(mixed_s, output_weight) + offset[:high]).astype(BF)
        part_0, normed_sent = lax.optimization_barrier((part_0, normed))
        normed_cols = my_columns(normed_sent)
        error_1 = (weight_s * group_sum(part_0, tensor_count)).astype(BF)

        back_u = mix_back(probs_s, mm_nt(error_1, output_weight).astype(BF)).astype(BF)
        upper_1 = (upper.astype(F32) - step_rate * mm(gram[:, :high], back_u)).astype(BF)
        mixed_q = mix(probs_q, upper_1).astype(BF)
        cross = (-step_rate * mm_nt(mixed_q, mixed_s)).astype(BF)
        part_1 = mm(mixed_q, output_weight) + mm(cross, error_1)
        part_1 = (part_1 + offset[low:]).astype(BF)
        error_2 = (weight_q * group_sum(part_1, tensor_count)).astype(BF)

        errors = (-step_rate * mm_nt(error_2, error_1)).astype(BF)
        back_z1 = (mm_nt(error_2, output_weight) + mm(errors, mixed_s)).astype(BF)
        back_u1 = mix_back(probs_q, back_z1)
        back_u1_b = back_u1.astype(BF)
        back_gram = (-step_rate * mm(gram[:high], back_u1_b)).astype(BF)
        second = mix(probs_s, back_gram).astype(BF)
        error_back = (mm(second, output_weight) + mm_tn(cross, error_2)).astype(BF)
        is_support = (position < split)[:, None]
        left = jnp.where(is_support, below(second, length), above(mixed_q, length))
        errors_both = jnp.where(is_support, below(error_1, length), above(error_2, length))
        error_back, normed_cols, errors_both, left = lax.optimization_barrier(
            (error_back, normed_cols, errors_both, left)
        )
        both_cols = my_columns(errors_both)
        left_all = gather_tokens(left)
        error_sum = group_sum(error_back, tensor_count)
        error_3 = (weight_s * error_sum).astype(BF)
        error_3_cols = my_columns(error_3)

        back_z0 = (mm_nt(error_3, output_weight) + mm_tn(errors, mixed_q)).astype(BF)
        late = mix_back(probs_s, back_z0)
        value_rows = (back_u1 + jnp.pad(late, ((0, length - high), (0, 0)))).astype(BF)
        value_rows_all = gather_by_copies(value_rows, 1)
        total_output = (
            mm_tn(left_all, both_cols)
            + mm_tn(mixed_s_all, error_3_cols)
        )
        total_value = mm_tn(normed_cols, value_rows_all)
        return (total_value, total_output)

    return per_device


def solution(mesh):
    return jax.shard_map(
        make_device(mesh.shape["tensor"]),
        mesh=mesh,
        in_specs=(
            P("task", "tensor"),
            P("task", "tensor"),
            P("task", "tensor"),
            P("task", "tensor"),
            P(None, "tensor"),
            P("tensor", None),
            P("task"),
        ),
        out_specs=(P("task", "tensor"), P("tensor", "task")),
        check_vma=False,
    )
```

```python
import functools

import jax
import jax.numpy as jnp
from jax import lax
from jax.experimental import pallas as pl
from jax.experimental.pallas import tpu as pltpu
from jax.sharding import PartitionSpec as P

HD = 128
BF = jnp.bfloat16
F32 = jnp.float32

step_rate = 0.25


def normed_rows(inputs):
    values = inputs.astype(F32)
    scale = lax.rsqrt(jnp.mean(values * values, axis=-1, keepdims=True) + 1e-05)
    return (values * scale).astype(BF)


def attention_probs(queries, key_rows, heads):
    length = queries.shape[0]
    query_h = queries.reshape(length, heads, -1)
    key_h = key_rows.reshape(length, heads, -1)
    scores = jnp.einsum("ihd,jhd->hij", query_h, key_h, preferred_element_type=F32)
    scores = scores / jnp.sqrt(F32(query_h.shape[2]))
    position = jnp.arange(length)
    causal = position[:, None] >= position[None, :]
    scores = jnp.where(causal[None], scores, F32(-1e30))
    scores = scores - jnp.max(scores, axis=-1, keepdims=True)
    expo = jnp.exp(scores)
    return (expo / jnp.sum(expo, axis=-1, keepdims=True)).astype(BF)


def mm(left, right):
    return jnp.dot(left, right, preferred_element_type=F32)


def mm_nt(left, right):
    return lax.dot_general(left, right, (((1,), (1,)), ((), ())), preferred_element_type=F32)


def mm_tn(left, right):
    return lax.dot_general(left, right, (((0,), (0,)), ((), ())), preferred_element_type=F32)


def mix(probs, rows):
    heads = probs.shape[0]
    split = rows.reshape(rows.shape[0], heads, -1)
    out = jnp.einsum("hij,jhd->ihd", probs, split, preferred_element_type=F32)
    return out.reshape(out.shape[0], -1)


def mix_back(probs, rows):
    heads = probs.shape[0]
    split = rows.reshape(rows.shape[0], heads, -1)
    out = jnp.einsum("hij,ihd->jhd", probs, split, preferred_element_type=F32)
    return out.reshape(out.shape[0], -1)


def group_sum(term, count):
    term = term.astype(BF)
    if count == 1:
        return term.astype(F32)
    if count == 2:
        other = lax.ppermute(term, "tensor", ((0, 1), (1, 0)))
        return term.astype(F32) + other.astype(F32)
    share = lax.psum_scatter(term, "tensor", scatter_dimension=1, tiled=True)
    return lax.all_gather(share, "tensor", axis=1, tiled=True).astype(F32)


def full_rows(inputs, count, index):
    if count != 2:
        return lax.all_gather(inputs, "tensor", axis=1, tiled=True)
    other = lax.ppermute(inputs, "tensor", ((0, 1), (1, 0)))
    low = jnp.where(index == 0, inputs, other)
    high = jnp.where(index == 0, other, inputs)
    return jnp.concatenate([low, high], axis=1)


def gather_kernel(lines, src_ref, out_ref, own_sem, send_sem, line_sem, side_sem, core_sem):
    me = lax.axis_index("task")
    core, side, line = lax.rem(me, 2), lax.rem(me // 2, 2), me // 4

    def place(back, over_side, over_core):
        line_from = lax.rem(line + lines - back, lines)
        side_from = 1 - side if over_side else side
        core_from = 1 - core if over_core else core
        return (line_from * 2 + side_from) * 2 + core_from

    side_peer, core_peer = place(0, True, False), place(0, False, True)
    peers = [place(lines - step, False, False) for step in range(1, lines)] + [side_peer, core_peer]
    barrier = pltpu.get_barrier_semaphore()
    for peer in peers:
        pl.semaphore_signal(
            barrier, inc=1, device_id={"task": peer}, device_id_type=pl.DeviceIdType.MESH
        )
    pl.semaphore_wait(barrier, len(peers))

    started = []

    def send(source, slot, arrival, peer):
        copy = pltpu.make_async_remote_copy(
            src_ref=source,
            dst_ref=out_ref.at[slot],
            send_sem=send_sem.at[len(started)],
            recv_sem=arrival,
            device_id={"task": peer},
            device_id_type=pl.DeviceIdType.MESH,
        )
        copy.start()
        started.append(copy)

    def arrived(slot, arrival, peer):
        pltpu.make_async_remote_copy(
            src_ref=out_ref.at[slot],
            dst_ref=out_ref.at[slot],
            send_sem=send_sem.at[0],
            recv_sem=arrival,
            device_id={"task": peer},
            device_id_type=pl.DeviceIdType.MESH,
        ).wait_recv()

    for step in sorted(range(1, lines), key=lambda step: -min(step, lines - step)):
        send(src_ref, me, line_sem.at[step], peers[step - 1])
    send(src_ref, me, side_sem.at[0], side_peer)
    send(src_ref, me, core_sem.at[0, 0], core_peer)
    own = pltpu.make_async_copy(src_ref, out_ref.at[me], own_sem)
    own.start()
    order = sorted(range(1, lines), key=lambda step: min(step, lines - step))
    for step in order:
        slot = place(step, False, False)
        arrived(slot, line_sem.at[step], side_peer)
        send(out_ref.at[slot], slot, side_sem.at[step], side_peer)
        send(out_ref.at[slot], slot, core_sem.at[step, 0], core_peer)
    for step in [0] + order:
        slot = place(step, True, False)
        arrived(slot, side_sem.at[step], side_peer)
        send(out_ref.at[slot], slot, core_sem.at[step, 1], core_peer)
    for step in [0] + order:
        for over in range(2):
            arrived(place(step, over == 1, True), core_sem.at[step, over], core_peer)
    own.wait()
    for copy in started:
        copy.wait_send()


def gather_by_copies(rows, number):
    count = lax.axis_size("task")
    if count % 4:
        return gather_tokens(rows)
    lines = count // 4
    sends = (lines + 1) + 2 * (lines - 1) + lines
    gathered = pl.pallas_call(
        functools.partial(gather_kernel, lines),
        out_shape=jax.ShapeDtypeStruct((count,) + rows.shape, rows.dtype),
        in_specs=[pl.BlockSpec(memory_space=pltpu.VMEM)],
        out_specs=pl.BlockSpec(memory_space=pltpu.VMEM),
        scratch_shapes=[
            pltpu.SemaphoreType.DMA,
            pltpu.SemaphoreType.DMA((sends,)),
            pltpu.SemaphoreType.DMA((lines,)),
            pltpu.SemaphoreType.DMA((lines,)),
            pltpu.SemaphoreType.DMA((lines, 2)),
        ],
        compiler_params=pltpu.CompilerParams(collective_id=number, has_side_effects=True),
        cost_estimate=pl.CostEstimate(
            flops=0, bytes_accessed=16 * rows.size * rows.dtype.itemsize * count, transcendentals=0
        ),
    )(rows)
    return gathered.reshape(count * rows.shape[0], rows.shape[1])


def gather_tokens(rows):
    return lax.all_gather(rows, "task", axis=0, tiled=True)


def my_columns(rows):
    return lax.all_to_all(rows, "task", split_axis=1, concat_axis=0, tiled=True)


def below(rows, length):
    return jnp.pad(rows, ((0, length - rows.shape[0]), (0, 0)))


def above(rows, length):
    return jnp.pad(rows, ((length - rows.shape[0], 0), (0, 0)))


def make_device(tensor_count):
    def per_device(inputs, targets, queries, key_rows, value_weight, output_weight, splits):
        length = inputs.shape[0]
        low, high = length // 4, 3 * length // 4
        heads = queries.shape[1] // HD
        index = lax.axis_index("tensor")
        normed = normed_rows(full_rows(inputs, tensor_count, index))
        offset_here = inputs.astype(F32) - targets.astype(F32)
        offset = jnp.concatenate(
            [jnp.where(index == block, offset_here, F32(0.0)) for block in range(tensor_count)],
            axis=1,
        )
        probs = attention_probs(queries, key_rows, heads)
        probs_s = probs[:, :high, :high]
        probs_q = probs[:, low:, :]
        split = splits[0]
        count_s = split.astype(F32)
        position = jnp.arange(length)
        support = (position < split).astype(F32)[:, None]
        weight_s = (support / count_s)[:high]
        weight_q = ((1.0 - support) / (F32(length) - count_s))[low:]

        upper = mm(normed, value_weight).astype(BF)
        mixed_s = mix(probs_s, upper[:high]).astype(BF)
        gram = mm_nt(normed, normed).astype(BF)
        mixed_s_all = gather_tokens(mixed_s)
        part_0 = (mm(mixed_s, output_weight) + offset[:high]).astype(BF)
        part_0, normed_sent = lax.optimization_barrier((part_0, normed))
        normed_cols = my_columns(normed_sent)
        error_1 = (weight_s * group_sum(part_0, tensor_count)).astype(BF)

        back_u = mix_back(probs_s, mm_nt(error_1, output_weight).astype(BF)).astype(BF)
        upper_1 = (upper.astype(F32) - step_rate * mm(gram[:, :high], back_u)).astype(BF)
        mixed_q = mix(probs_q, upper_1).astype(BF)
        cross = (-step_rate * mm_nt(mixed_q, mixed_s)).astype(BF)
        part_1 = mm(mixed_q, output_weight) + mm(cross, error_1)
        part_1 = (part_1 + offset[low:]).astype(BF)
        error_2 = (weight_q * group_sum(part_1, tensor_count)).astype(BF)

        errors = (-step_rate * mm_nt(error_2, error_1)).astype(BF)
        back_z1 = (mm_nt(error_2, output_weight) + mm(errors, mixed_s)).astype(BF)
        back_u1 = mix_back(probs_q, back_z1)
        back_u1_b = back_u1.astype(BF)
        back_gram = (-step_rate * mm(gram[:high], back_u1_b)).astype(BF)
        second = mix(probs_s, back_gram).astype(BF)
        error_back = (mm(second, output_weight) + mm_tn(cross, error_2)).astype(BF)
        is_support = (position < split)[:, None]
        left = jnp.where(is_support, below(second, length), above(mixed_q, length))
        errors_both = jnp.where(is_support, below(error_1, length), above(error_2, length))
        error_back, normed_cols, errors_both, left = lax.optimization_barrier(
            (error_back, normed_cols, errors_both, left)
        )
        both_cols = my_columns(errors_both)
        left, mixed_s_all = lax.optimization_barrier((left, mixed_s_all))
        left_all = gather_tokens(left)
        error_sum = group_sum(error_back, tensor_count)
        error_3 = (weight_s * error_sum).astype(BF)
        error_3_cols = my_columns(error_3)

        back_z0 = (mm_nt(error_3, output_weight) + mm_tn(errors, mixed_q)).astype(BF)
        late = mix_back(probs_s, back_z0)
        value_rows = (back_u1 + jnp.pad(late, ((0, length - high), (0, 0)))).astype(BF)
        value_rows_all = gather_by_copies(value_rows, 1)
        total_output = (
            mm_tn(left_all, both_cols)
            + mm_tn(mixed_s_all, error_3_cols)
        )
        total_value = mm_tn(normed_cols, value_rows_all)
        return (total_value, total_output)

    return per_device


def solution(mesh):
    return jax.shard_map(
        make_device(mesh.shape["tensor"]),
        mesh=mesh,
        in_specs=(
            P("task", "tensor"),
            P("task", "tensor"),
            P("task", "tensor"),
            P("task", "tensor"),
            P(None, "tensor"),
            P("tensor", None),
            P("task"),
        ),
        out_specs=(P("task", "tensor"), P("tensor", "task")),
        check_vma=False,
    )
```
